256 devices in a mesh: scan: 2 (over y), slab: 128 (over z, x, core).
Axes of the slice: x: 4, y: 2, z: 16, core: 2. Of those that a mesh axis runs over, the one named last changes fastest.
The devices are a block of a 4x16x16 slice.
Arguments:
- image: float32 [2, 128, 256, 128], P(None, 'slab', 'scan'), parts along dimension 2, may hold values from -6 to 6
- sensitivity: bfloat16 [12, 2, 128, 128, 128], P('scan', None, 'slab'), parts along dimension 0, may hold values from -1.5 to 1.5
- kernel: float32 [256, 256, 256], P(None, 'slab'), may hold values from 0.1 to 4
Outputs:
- normal_image: float32 [2, 128, 256, 128], P(None, 'slab', 'scan'), parts along dimension 2
The draws below stay inside these ranges and needn't reach their ends.
There are 2 independent parts, one for each index of `scan`. The reference program is written for one: setup_inputs(seed, part) draws one part's arguments, and reference() takes and returns one part's arrays. A program takes and returns all parts, laid end to end along the dimension named above; an argument that names none is the same for every part. Nothing has to cross between parts.
All inputs are finite; a program needn't handle non-finite values.
Results may differ from the reference program's by a relative error of at most 0.0024.
Values may be sent and summed in bfloat16 or wider, within the bound.
A program may use at most 64 MiB of HBM per device.

```python
import math
import jax
import jax.numpy as jnp
from jax import lax

NX = 128
NY = 128
NZ = 128
COILS = 6
GX = 256
GY = 256
GZ = 256


def block_levels(key, shape, pieces, smallest, top_value):
    level, own = 1.0, jax.random.fold_in(key, 6)
    for dim, shards_of in pieces:
        draws = jnp.exp(jax.random.uniform(jax.random.fold_in(own, dim), (shards_of,), jnp.float32, smallest / len(pieces), top_value / len(pieces)))
        level = level * jnp.repeat(draws, shape[dim] // shards_of).reshape([-1 if axis == dim else 1 for axis in range(len(shape))])
    return level


def gaussian(own_key, extent, deviation, bound, cuts=(), held_as=jnp.bfloat16):
    values = deviation * jax.random.normal(own_key, extent, jnp.float32)
    if cuts:
        values = values * block_levels(own_key, extent, cuts, -0.22, 0.18)
    return jnp.clip(values, -bound, bound).astype(held_as)


def setup_inputs(seed: int = 0, part: int = 0) -> dict:
    streams_of = jax.random.split(jax.random.key(seed), 4)
    part_splits = jax.random.split(jax.random.fold_in(streams_of[3], part), 4)
    return {
        "image": gaussian(part_splits[0], (2, NX, NY, NZ), 1.0, 6.0, ((1, 128),), jnp.float32),
        "sensitivity": gaussian(part_splits[1], (COILS, 2, NX, NY, NZ), 0.25, 1.5, ((2, 128),)),
        "kernel": jnp.clip(jnp.exp(math.log(4.0) - 3.6888794 * jax.random.uniform(streams_of[2], (GX, GY, GZ), jnp.float32) ** block_levels(streams_of[2], (GX, GY, GZ), ((1, 128),), -0.2, 0.2)), 0.1, 4.0),
    }


smooth_weight = 0.1

def fourier_table(count_out, count_in, length, sign_value):
    row_index = lax.broadcasted_iota(jnp.int32, (count_out, count_in), 0)
    column_index = lax.broadcasted_iota(jnp.int32, (count_out, count_in), 1)
    phases = row_index * column_index % length
    angles = phases.astype(jnp.float32) * (2.0 * math.pi / length)
    factor = 1.0 / math.sqrt(length)
    real_part = jnp.cos(angles) * factor
    imaginary = sign_value * jnp.sin(angles) * factor
    stacked = jnp.stack([jnp.stack([real_part, -imaginary]), jnp.stack([imaginary, real_part])])
    return stacked.astype(jnp.bfloat16)

def transform(matrix, values, pattern):
    return jnp.einsum(pattern, matrix.astype(jnp.float32), values.astype(jnp.float32))

def reference(image, sensitivity, kernel):
    forward_first = fourier_table(GX, NX, GX, -1.0)
    forward_second = fourier_table(GY, NY, GY, -1.0)
    forward_third = fourier_table(GZ, NZ, GZ, -1.0)
    inverse_first = fourier_table(NX, GX, GX, 1.0)
    inverse_second = fourier_table(NY, GY, GY, 1.0)
    inverse_third = fourier_table(NZ, GZ, GZ, 1.0)

    def one_coil(accumulated, coil_maps):
        coil_real = coil_maps[0].astype(jnp.float32)
        coil_imaginary = coil_maps[1].astype(jnp.float32)
        coil_image = jnp.stack([coil_real * image[0] - coil_imaginary * image[1], coil_real * image[1] + coil_imaginary * image[0]]).astype(jnp.bfloat16)
        along_second = transform(forward_second, coil_image, 'pqkj,qajb->pakb').astype(jnp.bfloat16)
        along_third = transform(forward_third, along_second, 'pqkj,qabj->pabk').astype(jnp.bfloat16)
        spectrum = transform(forward_first, along_third, 'pqkj,qjab->pkab')
        filtered = (spectrum * kernel).astype(jnp.bfloat16)
        back_first = transform(inverse_first, filtered, 'pqkj,qjab->pkab').astype(jnp.bfloat16)
        back_third = transform(inverse_third, back_first, 'pqkj,qabj->pabk').astype(jnp.bfloat16)
        coil_result = transform(inverse_second, back_third, 'pqkj,qajb->pakb')
        accumulated = accumulated + jnp.stack([coil_real * coil_result[0] + coil_imaginary * coil_result[1], coil_real * coil_result[1] - coil_imaginary * coil_result[0]])
        return (accumulated, None)
    accumulated = lax.scan(one_coil, jnp.zeros(image.shape, jnp.float32), sensitivity)[0]
    padded = jnp.pad(image, ((0, 0), (1, 1), (1, 1), (1, 1)))
    beside = padded[:, 2:, 1:-1, 1:-1] + padded[:, :-2, 1:-1, 1:-1]
    beside = beside + padded[:, 1:-1, 2:, 1:-1] + padded[:, 1:-1, :-2, 1:-1]
    beside = beside + padded[:, 1:-1, 1:-1, 2:] + padded[:, 1:-1, 1:-1, :-2]
    penalty = 6.0 * image - beside
    return accumulated + smooth_weight * penalty
```

```python
import functools
import math

import jax
import jax.numpy as jnp
import ml_dtypes
import numpy as np
from jax import lax
from jax.experimental import pallas as pl
from jax.experimental.pallas import tpu as pltpu
from jax.sharding import PartitionSpec as P

MESH = pl.DeviceIdType.MESH
smooth_weight = 0.1


def factor(count_out, count_in, length, sign):
    phases = np.outer(np.arange(count_out), np.arange(count_in)) % length
    angles = phases.astype(np.float32) * np.float32(2.0 * math.pi / length)
    scale = np.float32(1.0 / math.sqrt(length))
    return np.cos(angles) * scale, sign * np.sin(angles) * scale


def stacked(real, imaginary):
    rows = np.stack([np.stack([real, -imaginary], 1), np.stack([imaginary, real], 1)])
    return rows.astype(ml_dtypes.bfloat16)


def tables(nx, ny, nz, gx, gy, gz):
    fx, fy, fz = (stacked(*factor(g, n, g, -1.0)) for n, g in ((nx, gx), (ny, gy), (nz, gz)))
    hx, hy, hz = (stacked(*factor(n, g, g, 1.0)) for n, g in ((nx, gx), (ny, gy), (nz, gz)))
    return (
        fy.transpose(1, 0, 2, 3).reshape(2 * gy, 2 * ny),
        fx.transpose(0, 1, 3, 2).reshape(2 * gx, 2 * nx),
        fz.transpose(2, 3, 0, 1).reshape(2 * nz, 2 * gz),
        hz.transpose(2, 3, 0, 1).reshape(2 * gz, 2 * nz),
        hx.transpose(1, 0, 2, 3).reshape(2 * nx, 2 * gx),
        hy.transpose(0, 1, 3, 2).reshape(2 * ny, 2 * gy),
    )


def dot(a, b):
    return jnp.dot(a, b, preferred_element_type=jnp.float32)


def body(
    n,
    image_hbm,
    maps_hbm,
    kernel_hbm,
    *refs,
):
    table_hbm, refs = refs[:6], refs[6:]
    (out, image, maps, weight, *refs) = refs
    table, refs = refs[:6], refs[6:]
    (lines, spectra, backs, planes, face, halo, total, load_sem, out_sem, in_sem, back_out_sem, back_in_sem, face_sem, halo_sem) = refs
    coils, _, ny, nz = maps.shape
    per = lines.shape[2]
    me = lax.axis_index("slab")

    loads = [pltpu.make_async_copy(image_hbm.at[:, 0], image, load_sem.at[0])]
    loads.append(pltpu.make_async_copy(maps_hbm.at[:, :, 0], maps, load_sem.at[1]))
    for i in range(6):
        loads.append(pltpu.make_async_copy(table_hbm[i], table[i], load_sem.at[2 + i]))
    for i in range(per):
        loads.append(pltpu.make_async_copy(kernel_hbm.at[:, i], weight.at[i], load_sem.at[8 + i]))
    for load in loads:
        load.start()

    barrier = pltpu.get_barrier_semaphore()

    def greet(k, carry):
        pl.semaphore_signal(
            barrier, inc=1, device_id={"slab": lax.rem(me + k, n)}, device_id_type=MESH
        )
        return carry

    lax.fori_loop(1, n, greet, 0)

    for load in loads[:3]:
        load.wait()
    face[...] = image[...].astype(face.dtype)

    def spread(c, carry):
        real, imaginary = maps[c, 0].astype(jnp.float32), maps[c, 1].astype(jnp.float32)
        coil_real = real * image[0] - imaginary * image[1]
        coil_imaginary = real * image[1] + imaginary * image[0]
        coil = jnp.concatenate([coil_real, coil_imaginary]).astype(jnp.bfloat16)
        along = dot(table[0][...], coil).astype(jnp.bfloat16)
        lines.at[c].reshape(n * per * 2, nz)[...] = along
        spectra[c, :, me] = lines[c, me]
        return carry

    lax.fori_loop(0, coils, spread, 0)
    pl.semaphore_wait(barrier, n - 1)

    def send(c, d):
        pltpu.make_async_remote_copy(
            lines.at[c, d],
            spectra.at[c, :, me],
            out_sem.at[c],
            in_sem.at[c],
            device_id={"slab": d},
            device_id_type=MESH,
        ).start()

    def send_back(c, d):
        pltpu.make_async_remote_copy(
            backs.at[c, :, d],
            planes.at[c, me],
            back_out_sem.at[c],
            back_in_sem.at[c],
            device_id={"slab": d},
            device_id_type=MESH,
        ).start()

    def each(act, c):
        def step(k, carry):
            act(c, lax.rem(me + k, n))
            return carry

        lax.fori_loop(1, n, step, 0)

    def face_copy(side):
        return pltpu.make_async_remote_copy(
            face,
            halo.at[side],
            face_sem.at[side],
            halo_sem.at[side],
            device_id={"slab": lax.rem(me + (1 if side == 0 else n - 1), n)},
            device_id_type=MESH,
        )

    @pl.when(me < n - 1)
    def _():
        face_copy(0).start()

    @pl.when(me > 0)
    def _():
        face_copy(1).start()

    def start(c, carry):
        each(send, c)
        return carry

    lax.fori_loop(0, coils, start, 0)
    for load in loads[3:]:
        load.wait()

    def middle(c, carry):
        arrived = spectra.at[c, :, pl.ds(0, n - 1)]
        pltpu.make_async_copy(arrived, arrived, in_sem.at[c]).wait()
        for i in range(per):
            x = spectra.at[c, i].reshape(2 * n, nz)[...]
            along = dot(table[1][...], x).astype(jnp.bfloat16)
            half = along.shape[0] // 2
            rows = jnp.concatenate([along[:half], along[half:]], axis=1)
            spectrum = dot(rows, table[2][...])
            gz = spectrum.shape[1] // 2
            k = weight[i]
            filtered = jnp.concatenate(
                [spectrum[:, :gz] * k, spectrum[:, gz:] * k], axis=1
            ).astype(jnp.bfloat16)
            back = dot(filtered, table[3][...]).astype(jnp.bfloat16)
            columns = jnp.concatenate([back[:, :nz], back[:, nz:]], axis=0)
            first = dot(table[4][...], columns).astype(jnp.bfloat16)
            backs.at[c, i].reshape(2 * n, nz)[...] = first
        planes[c, me] = backs[c, :, me]
        each(send_back, c)
        return carry

    lax.fori_loop(0, coils, middle, 0)

    @pl.when(me > 0)
    def _():
        face_copy(0).wait_recv()

    @pl.when(me == 0)
    def _():
        halo[0] = jnp.zeros_like(halo[0])

    @pl.when(me < n - 1)
    def _():
        face_copy(1).wait_recv()

    @pl.when(me == n - 1)
    def _():
        halo[1] = jnp.zeros_like(halo[1])

    for p in range(2):
        plane = image[p]
        beside = halo[0, p].astype(jnp.float32) + halo[1, p].astype(jnp.float32)
        row, column = jnp.zeros((1, nz), jnp.float32), jnp.zeros((ny, 1), jnp.float32)
        beside += jnp.concatenate([plane[1:], row], axis=0) + jnp.concatenate([row, plane[:-1]], axis=0)
        beside += jnp.concatenate([plane[:, 1:], column], axis=1) + jnp.concatenate([column, plane[:, :-1]], axis=1)
        total[p] = smooth_weight * (6.0 * plane - beside)

    def finish(c, carry):
        arrived = planes.at[c, pl.ds(0, n - 1)]
        pltpu.make_async_copy(arrived, arrived, back_in_sem.at[c]).wait()
        coil = dot(table[5][...], planes.at[c].reshape(n * per * 2, nz)[...])
        coil_real, coil_imaginary = coil[:ny], coil[ny:]
        real, imaginary = maps[c, 0].astype(jnp.float32), maps[c, 1].astype(jnp.float32)
        total[0] += real * coil_real + imaginary * coil_imaginary
        total[1] += real * coil_imaginary - imaginary * coil_real
        return carry

    lax.fori_loop(0, coils, finish, 0)
    out[:, 0] = total[...]

    def drain(c, carry):
        left = lines.at[c, pl.ds(0, n - 1)]
        pltpu.make_async_copy(left, left, out_sem.at[c]).wait()
        pltpu.make_async_copy(left, left, back_out_sem.at[c]).wait()
        return carry

    lax.fori_loop(0, coils, drain, 0)

    @pl.when(me < n - 1)
    def _():
        face_copy(0).wait_send()

    @pl.when(me > 0)
    def _():
        face_copy(1).wait_send()


def local(n, image, sensitivity, kernel):
    coils, _, _, ny, nz = sensitivity.shape
    gx, per, gz = kernel.shape
    nx, gy = n, n * per
    consts = [jnp.asarray(t) for t in tables(nx, ny, nz, gx, gy, gz)]
    whole = pl.BlockSpec(memory_space=pl.ANY)
    half = jnp.bfloat16
    return pl.pallas_call(
        functools.partial(body, n),
        out_shape=jax.ShapeDtypeStruct(image.shape, image.dtype),
        in_specs=[whole] * 9,
        out_specs=pl.BlockSpec(memory_space=pltpu.VMEM),
        scratch_shapes=[
            pltpu.VMEM((2, ny, nz), jnp.float32),
            pltpu.VMEM((coils, 2, ny, nz), half),
            pltpu.VMEM((per, gx, gz), jnp.float32),
            *[pltpu.VMEM(t.shape, half) for t in consts],
            pltpu.VMEM((coils, n, per, 2, nz), half),
            pltpu.VMEM((coils, per, n, 2, nz), half),
            pltpu.VMEM((coils, per, n, 2, nz), half),
            pltpu.VMEM((coils, n, per, 2, nz), half),
            pltpu.VMEM((2, ny, nz), half),
            pltpu.VMEM((2, 2, ny, nz), half),
            pltpu.VMEM((2, ny, nz), jnp.float32),
            pltpu.SemaphoreType.DMA((8 + per,)),
            pltpu.SemaphoreType.DMA((coils,)),
            pltpu.SemaphoreType.DMA((coils,)),
            pltpu.SemaphoreType.DMA((coils,)),
            pltpu.SemaphoreType.DMA((coils,)),
            pltpu.SemaphoreType.DMA((2,)),
            pltpu.SemaphoreType.DMA((2,)),
        ],
        compiler_params=pltpu.CompilerParams(collective_id=0, has_side_effects=True),
        name="normal_operator",
    )(image, sensitivity, kernel, *consts)


def solution(mesh):
    return jax.shard_map(
        functools.partial(local, mesh.shape["slab"]),
        mesh=mesh,
        in_specs=(
            P(None, "slab", "scan", None),
            P("scan", None, "slab", None, None),
            P(None, "slab", None),
        ),
        out_specs=P(None, "slab", "scan", None),
        check_vma=False,
    )
```

```python
import functools
import math

import jax
import jax.numpy as jnp
import ml_dtypes
import numpy as np
from jax import lax
from jax.experimental import pallas as pl
from jax.experimental.pallas import tpu as pltpu
from jax.sharding import PartitionSpec as P

MESH = pl.DeviceIdType.MESH
smooth_weight = 0.1
group = 3


def factor(count_out, count_in, length, sign):
    phases = np.outer(np.arange(count_out), np.arange(count_in)) % length
    angles = phases.astype(np.float32) * np.float32(2.0 * math.pi / length)
    scale = np.float32(1.0 / math.sqrt(length))
    return np.cos(angles) * scale, sign * np.sin(angles) * scale


def stacked(real, imaginary):
    rows = np.stack([np.stack([real, -imaginary], 1), np.stack([imaginary, real], 1)])
    return rows.astype(ml_dtypes.bfloat16)


def tables(nx, ny, nz, gx, gy, gz):
    fx, fy, fz = (stacked(*factor(g, n, g, -1.0)) for n, g in ((nx, gx), (ny, gy), (nz, gz)))
    hx, hy, hz = (stacked(*factor(n, g, g, 1.0)) for n, g in ((nx, gx), (ny, gy), (nz, gz)))
    return (
        fy.transpose(1, 0, 2, 3).reshape(2 * gy, 2 * ny),
        fx.transpose(0, 1, 3, 2).reshape(2 * gx, 2 * nx),
        fz.transpose(2, 3, 0, 1).reshape(2 * nz, 2 * gz),
        hz.transpose(2, 3, 0, 1).reshape(2 * gz, 2 * nz),
        hx.transpose(1, 0, 2, 3).reshape(2 * nx, 2 * gx),
        hy.transpose(0, 1, 3, 2).reshape(2 * ny, 2 * gy),
    )


def dot(a, b):
    return jnp.dot(a, b, preferred_element_type=jnp.float32)


def body(
    n,
    image_hbm,
    maps_hbm,
    kernel_hbm,
    *refs,
):
    table_hbm, refs = refs[:6], refs[6:]
    (out, image, maps, weight, *refs) = refs
    table, refs = refs[:6], refs[6:]
    (lines, spectra, backs, planes, face, halo, total, load_sem, out_sem, in_sem, back_out_sem, back_in_sem, face_sem, halo_sem) = refs
    coils, _, ny, nz = maps.shape
    per = lines.shape[2]
    me = lax.axis_index("slab")

    loads = [pltpu.make_async_copy(image_hbm.at[:, 0], image, load_sem.at[0])]
    loads.append(pltpu.make_async_copy(maps_hbm.at[:, :, 0], maps, load_sem.at[1]))
    for i in range(6):
        loads.append(pltpu.make_async_copy(table_hbm[i], table[i], load_sem.at[2 + i]))
    for i in range(per):
        loads.append(pltpu.make_async_copy(kernel_hbm.at[:, i], weight.at[i], load_sem.at[8 + i]))
    for load in loads:
        load.start()

    barrier = pltpu.get_barrier_semaphore()

    def greet(k, carry):
        pl.semaphore_signal(
            barrier, inc=1, device_id={"slab": lax.rem(me + k, n)}, device_id_type=MESH
        )
        return carry

    lax.fori_loop(1, n, greet, 0)

    for load in loads[:3]:
        load.wait()
    face[...] = image[...].astype(face.dtype)

    def spread(c, carry):
        real, imaginary = maps[c, 0].astype(jnp.float32), maps[c, 1].astype(jnp.float32)
        coil_real = real * image[0] - imaginary * image[1]
        coil_imaginary = real * image[1] + imaginary * image[0]
        coil = jnp.concatenate([coil_real, coil_imaginary]).astype(jnp.bfloat16)
        along = dot(table[0][...], coil).astype(jnp.bfloat16)
        lines.at[c].reshape(n * per * 2, nz)[...] = along
        spectra[c, :, me] = lines[c, me]
        return carry

    lax.fori_loop(0, coils, spread, 0)
    pl.semaphore_wait(barrier, n - 1)

    def send(g, d):
        pltpu.make_async_remote_copy(
            lines.at[pl.ds(g * group, group), d],
            spectra.at[pl.ds(g * group, group), :, me],
            out_sem.at[g],
            in_sem.at[g],
            device_id={"slab": d},
            device_id_type=MESH,
        ).start()

    def send_back(g, d):
        pltpu.make_async_remote_copy(
            backs.at[pl.ds(g * group, group), :, d],
            planes.at[pl.ds(g * group, group), me],
            back_out_sem.at[g],
            back_in_sem.at[g],
            device_id={"slab": d},
            device_id_type=MESH,
        ).start()

    def each(act, g):
        def step(k, carry):
            act(g, lax.rem(me + k, n))
            return carry

        lax.fori_loop(1, n, step, 0)

    def face_copy(side):
        return pltpu.make_async_remote_copy(
            face,
            halo.at[side],
            face_sem.at[side],
            halo_sem.at[side],
            device_id={"slab": lax.rem(me + (1 if side == 0 else n - 1), n)},
            device_id_type=MESH,
        )

    @pl.when(me < n - 1)
    def _():
        face_copy(0).start()

    @pl.when(me > 0)
    def _():
        face_copy(1).start()

    groups = coils // group

    def start(g, carry):
        each(send, g)
        return carry

    lax.fori_loop(0, groups, start, 0)
    for load in loads[3:]:
        load.wait()

    def middle(c, carry):
        for i in range(per):
            x = spectra.at[c, i].reshape(2 * n, nz)[...]
            along = dot(table[1][...], x).astype(jnp.bfloat16)
            half = along.shape[0] // 2
            rows = jnp.concatenate([along[:half], along[half:]], axis=1)
            spectrum = dot(rows, table[2][...])
            gz = spectrum.shape[1] // 2
            k = weight[i]
            filtered = jnp.concatenate(
                [spectrum[:, :gz] * k, spectrum[:, gz:] * k], axis=1
            ).astype(jnp.bfloat16)
            back = dot(filtered, table[3][...]).astype(jnp.bfloat16)
            columns = jnp.concatenate([back[:, :nz], back[:, nz:]], axis=0)
            first = dot(table[4][...], columns).astype(jnp.bfloat16)
            backs.at[c, i].reshape(2 * n, nz)[...] = first
        planes[c, me] = backs[c, :, me]
        return carry

    def turn(g, carry):
        arrived = spectra.at[pl.ds(g * group, group), :, pl.ds(0, n - 1)]
        pltpu.make_async_copy(arrived, arrived, in_sem.at[g]).wait()
        lax.fori_loop(g * group, (g + 1) * group, middle, 0)
        each(send_back, g)
        return carry

    lax.fori_loop(0, groups, turn, 0)

    @pl.when(me > 0)
    def _():
        face_copy(0).wait_recv()

    @pl.when(me == 0)
    def _():
        halo[0] = jnp.zeros_like(halo[0])

    @pl.when(me < n - 1)
    def _():
        face_copy(1).wait_recv()

    @pl.when(me == n - 1)
    def _():
        halo[1] = jnp.zeros_like(halo[1])

    for p in range(2):
        plane = image[p]
        beside = halo[0, p].astype(jnp.float32) + halo[1, p].astype(jnp.float32)
        row, column = jnp.zeros((1, nz), jnp.float32), jnp.zeros((ny, 1), jnp.float32)
        beside += jnp.concatenate([plane[1:], row], axis=0) + jnp.concatenate([row, plane[:-1]], axis=0)
        beside += jnp.concatenate([plane[:, 1:], column], axis=1) + jnp.concatenate([column, plane[:, :-1]], axis=1)
        total[p] = smooth_weight * (6.0 * plane - beside)

    def finish(c, carry):
        coil = dot(table[5][...], planes.at[c].reshape(n * per * 2, nz)[...])
        coil_real, coil_imaginary = coil[:ny], coil[ny:]
        real, imaginary = maps[c, 0].astype(jnp.float32), maps[c, 1].astype(jnp.float32)
        total[0] += real * coil_real + imaginary * coil_imaginary
        total[1] += real * coil_imaginary - imaginary * coil_real
        return carry

    def gather(g, carry):
        arrived = planes.at[pl.ds(g * group, group), pl.ds(0, n - 1)]
        pltpu.make_async_copy(arrived, arrived, back_in_sem.at[g]).wait()
        return lax.fori_loop(g * group, (g + 1) * group, finish, carry)

    lax.fori_loop(0, groups, gather, 0)
    out[:, 0] = total[...]

    def drain(g, carry):
        left = lines.at[pl.ds(g * group, group), pl.ds(0, n - 1)]
        pltpu.make_async_copy(left, left, out_sem.at[g]).wait()
        pltpu.make_async_copy(left, left, back_out_sem.at[g]).wait()
        return carry

    lax.fori_loop(0, groups, drain, 0)

    @pl.when(me < n - 1)
    def _():
        face_copy(0).wait_send()

    @pl.when(me > 0)
    def _():
        face_copy(1).wait_send()


def local(n, image, sensitivity, kernel):
    coils, _, _, ny, nz = sensitivity.shape
    gx, per, gz = kernel.shape
    nx, gy = n, n * per
    consts = [jnp.asarray(t) for t in tables(nx, ny, nz, gx, gy, gz)]
    whole = pl.BlockSpec(memory_space=pl.ANY)
    half = jnp.bfloat16
    return pl.pallas_call(
        functools.partial(body, n),
        out_shape=jax.ShapeDtypeStruct(image.shape, image.dtype),
        in_specs=[whole] * 9,
        out_specs=pl.BlockSpec(memory_space=pltpu.VMEM),
        scratch_shapes=[
            pltpu.VMEM((2, ny, nz), jnp.float32),
            pltpu.VMEM((coils, 2, ny, nz), half),
            pltpu.VMEM((per, gx, gz), jnp.float32),
            *[pltpu.VMEM(t.shape, half) for t in consts],
            pltpu.VMEM((coils, n, per, 2, nz), half),
            pltpu.VMEM((coils, per, n, 2, nz), half),
            pltpu.VMEM((coils, per, n, 2, nz), half),
            pltpu.VMEM((coils, n, per, 2, nz), half),
            pltpu.VMEM((2, ny, nz), half),
            pltpu.VMEM((2, 2, ny, nz), half),
            pltpu.VMEM((2, ny, nz), jnp.float32),
            pltpu.SemaphoreType.DMA((8 + per,)),
            pltpu.SemaphoreType.DMA((coils // group,)),
            pltpu.SemaphoreType.DMA((coils // group,)),
            pltpu.SemaphoreType.DMA((coils // group,)),
            pltpu.SemaphoreType.DMA((coils // group,)),
            pltpu.SemaphoreType.DMA((2,)),
            pltpu.SemaphoreType.DMA((2,)),
        ],
        compiler_params=pltpu.CompilerParams(collective_id=0, has_side_effects=True),
        name="normal_operator",
    )(image, sensitivity, kernel, *consts)


def solution(mesh):
    return jax.shard_map(
        functools.partial(local, mesh.shape["slab"]),
        mesh=mesh,
        in_specs=(
            P(None, "slab", "scan", None),
            P("scan", None, "slab", None, None),
            P(None, "slab", None),
        ),
        out_specs=P(None, "slab", "scan", None),
        check_vma=False,
    )
```

```python
import functools
import math

import jax
import jax.numpy as jnp
import ml_dtypes
import numpy as np
from jax import lax
from jax.experimental import pallas as pl
from jax.experimental.pallas import tpu as pltpu
from jax.sharding import PartitionSpec as P

MESH = pl.DeviceIdType.MESH
smooth_weight = 0.1
group = 3


def factor(count_out, count_in, length, sign):
    phases = np.outer(np.arange(count_out), np.arange(count_in)) % length
    angles = phases.astype(np.float32) * np.float32(2.0 * math.pi / length)
    scale = np.float32(1.0 / math.sqrt(length))
    return np.cos(angles) * scale, sign * np.sin(angles) * scale


def stacked(real, imaginary):
    rows = np.stack([np.stack([real, -imaginary], 1), np.stack([imaginary, real], 1)])
    return rows.astype(ml_dtypes.bfloat16)


def tables(nx, ny, nz, gx, gy, gz):
    fx, fy, fz = (stacked(*factor(g, n, g, -1.0)) for n, g in ((nx, gx), (ny, gy), (nz, gz)))
    hx, hy, hz = (stacked(*factor(n, g, g, 1.0)) for n, g in ((nx, gx), (ny, gy), (nz, gz)))
    return (
        fy.transpose(1, 0, 2, 3).reshape(2 * gy, 2 * ny),
        fx.transpose(0, 1, 3, 2).reshape(2 * gx, 2 * nx),
        fz.transpose(2, 3, 0, 1).reshape(2 * nz, 2 * gz),
        hz.transpose(2, 3, 0, 1).reshape(2 * gz, 2 * nz),
        hx.transpose(1, 0, 2, 3).reshape(2 * nx, 2 * gx),
        hy.transpose(0, 1, 3, 2).reshape(2 * ny, 2 * gy),
    )


def dot(a, b):
    return jnp.dot(a, b, preferred_element_type=jnp.float32)


def body(
    n,
    image_hbm,
    maps_hbm,
    kernel_hbm,
    *refs,
):
    table_hbm, refs = refs[:6], refs[6:]
    (out, image, maps, weight, *refs) = refs
    table, refs = refs[:6], refs[6:]
    (lines, spectra, backs, planes, face, halo, total, load_sem, out_sem, in_sem, back_out_sem, back_in_sem, face_sem, halo_sem) = refs
    coils, _, ny, nz = maps.shape
    per = lines.shape[2]
    me = lax.axis_index("slab")

    loads = [pltpu.make_async_copy(image_hbm.at[:, 0], image, load_sem.at[0])]
    loads.append(pltpu.make_async_copy(maps_hbm.at[:, :, 0], maps, load_sem.at[1]))
    for i in range(6):
        loads.append(pltpu.make_async_copy(table_hbm[i], table[i], load_sem.at[2 + i]))
    for i in range(per):
        loads.append(pltpu.make_async_copy(kernel_hbm.at[:, i], weight.at[i], load_sem.at[8 + i]))
    for load in loads:
        load.start()

    barrier = pltpu.get_barrier_semaphore()

    def greet(k, carry):
        pl.semaphore_signal(
            barrier, inc=1, device_id={"slab": lax.rem(me + k, n)}, device_id_type=MESH
        )
        return carry

    lax.fori_loop(1, n, greet, 0, unroll=4)

    for load in loads[:3]:
        load.wait()
    face[...] = image[...].astype(face.dtype)

    def spread(c, carry):
        real, imaginary = maps[c, 0].astype(jnp.float32), maps[c, 1].astype(jnp.float32)
        coil_real = real * image[0] - imaginary * image[1]
        coil_imaginary = real * image[1] + imaginary * image[0]
        coil = jnp.concatenate([coil_real, coil_imaginary]).astype(jnp.bfloat16)
        along = dot(table[0][...], coil).astype(jnp.bfloat16)
        lines.at[c].reshape(n * per * 2, nz)[...] = along
        spectra[c, :, me] = lines[c, me]
        return carry

    lax.fori_loop(0, coils, spread, 0)
    pl.semaphore_wait(barrier, n - 1)

    def send(g, d):
        pltpu.make_async_remote_copy(
            lines.at[pl.ds(g * group, group), d],
            spectra.at[pl.ds(g * group, group), :, me],
            out_sem.at[g],
            in_sem.at[g],
            device_id={"slab": d},
            device_id_type=MESH,
        ).start()

    def send_back(g, d):
        pltpu.make_async_remote_copy(
            backs.at[pl.ds(g * group, group), :, d],
            planes.at[pl.ds(g * group, group), me],
            back_out_sem.at[g],
            back_in_sem.at[g],
            device_id={"slab": d},
            device_id_type=MESH,
        ).start()

    def each(act, g):
        def step(k, carry):
            act(g, lax.rem(me + k, n))
            return carry

        lax.fori_loop(1, n, step, 0, unroll=4)

    def face_copy(side):
        return pltpu.make_async_remote_copy(
            face,
            halo.at[side],
            face_sem.at[side],
            halo_sem.at[side],
            device_id={"slab": lax.rem(me + (1 if side == 0 else n - 1), n)},
            device_id_type=MESH,
        )

    @pl.when(me < n - 1)
    def _():
        face_copy(0).start()

    @pl.when(me > 0)
    def _():
        face_copy(1).start()

    groups = coils // group

    def start(g, carry):
        each(send, g)
        return carry

    lax.fori_loop(0, groups, start, 0)
    for load in loads[3:]:
        load.wait()

    def middle(c, carry):
        for i in range(per):
            x = spectra.at[c, i].reshape(2 * n, nz)[...]
            along = dot(table[1][...], x).astype(jnp.bfloat16)
            half = along.shape[0] // 2
            rows = jnp.concatenate([along[:half], along[half:]], axis=1)
            spectrum = dot(rows, table[2][...])
            gz = spectrum.shape[1] // 2
            k = weight[i]
            filtered = jnp.concatenate(
                [spectrum[:, :gz] * k, spectrum[:, gz:] * k], axis=1
            ).astype(jnp.bfloat16)
            back = dot(filtered, table[3][...]).astype(jnp.bfloat16)
            columns = jnp.concatenate([back[:, :nz], back[:, nz:]], axis=0)
            first = dot(table[4][...], columns).astype(jnp.bfloat16)
            backs.at[c, i].reshape(2 * n, nz)[...] = first
        planes[c, me] = backs[c, :, me]
        return carry

    def turn(g, carry):
        arrived = spectra.at[pl.ds(g * group, group), :, pl.ds(0, n - 1)]
        pltpu.make_async_copy(arrived, arrived, in_sem.at[g]).wait()
        lax.fori_loop(g * group, (g + 1) * group, middle, 0)
        each(send_back, g)
        return carry

    lax.fori_loop(0, groups, turn, 0)

    @pl.when(me > 0)
    def _():
        face_copy(0).wait_recv()

    @pl.when(me == 0)
    def _():
        halo[0] = jnp.zeros_like(halo[0])

    @pl.when(me < n - 1)
    def _():
        face_copy(1).wait_recv()

    @pl.when(me == n - 1)
    def _():
        halo[1] = jnp.zeros_like(halo[1])

    for p in range(2):
        plane = image[p]
        beside = halo[0, p].astype(jnp.float32) + halo[1, p].astype(jnp.float32)
        row, column = jnp.zeros((1, nz), jnp.float32), jnp.zeros((ny, 1), jnp.float32)
        beside += jnp.concatenate([plane[1:], row], axis=0) + jnp.concatenate([row, plane[:-1]], axis=0)
        beside += jnp.concatenate([plane[:, 1:], column], axis=1) + jnp.concatenate([column, plane[:, :-1]], axis=1)
        total[p] = smooth_weight * (6.0 * plane - beside)

    def finish(c, carry):
        coil = dot(table[5][...], planes.at[c].reshape(n * per * 2, nz)[...])
        coil_real, coil_imaginary = coil[:ny], coil[ny:]
        real, imaginary = maps[c, 0].astype(jnp.float32), maps[c, 1].astype(jnp.float32)
        total[0] += real * coil_real + imaginary * coil_imaginary
        total[1] += real * coil_imaginary - imaginary * coil_real
        return carry

    def gather(g, carry):
        arrived = planes.at[pl.ds(g * group, group), pl.ds(0, n - 1)]
        pltpu.make_async_copy(arrived, arrived, back_in_sem.at[g]).wait()
        return lax.fori_loop(g * group, (g + 1) * group, finish, carry)

    lax.fori_loop(0, groups, gather, 0)
    out[:, 0] = total[...]

    def drain(g, carry):
        left = lines.at[pl.ds(g * group, group), pl.ds(0, n - 1)]
        pltpu.make_async_copy(left, left, out_sem.at[g]).wait()
        pltpu.make_async_copy(left, left, back_out_sem.at[g]).wait()
        return carry

    lax.fori_loop(0, groups, drain, 0)

    @pl.when(me < n - 1)
    def _():
        face_copy(0).wait_send()

    @pl.when(me > 0)
    def _():
        face_copy(1).wait_send()


def local(n, image, sensitivity, kernel):
    coils, _, _, ny, nz = sensitivity.shape
    gx, per, gz = kernel.shape
    nx, gy = n, n * per
    consts = [jnp.asarray(t) for t in tables(nx, ny, nz, gx, gy, gz)]
    whole = pl.BlockSpec(memory_space=pl.ANY)
    half = jnp.bfloat16
    return pl.pallas_call(
        functools.partial(body, n),
        out_shape=jax.ShapeDtypeStruct(image.shape, image.dtype),
        in_specs=[whole] * 9,
        out_specs=pl.BlockSpec(memory_space=pltpu.VMEM),
        scratch_shapes=[
            pltpu.VMEM((2, ny, nz), jnp.float32),
            pltpu.VMEM((coils, 2, ny, nz), half),
            pltpu.VMEM((per, gx, gz), jnp.float32),
            *[pltpu.VMEM(t.shape, half) for t in consts],
            pltpu.VMEM((coils, n, per, 2, nz), half),
            pltpu.VMEM((coils, per, n, 2, nz), half),
            pltpu.VMEM((coils, per, n, 2, nz), half),
            pltpu.VMEM((coils, n, per, 2, nz), half),
            pltpu.VMEM((2, ny, nz), half),
            pltpu.VMEM((2, 2, ny, nz), half),
            pltpu.VMEM((2, ny, nz), jnp.float32),
            pltpu.SemaphoreType.DMA((8 + per,)),
            pltpu.SemaphoreType.DMA((coils // group,)),
            pltpu.SemaphoreType.DMA((coils // group,)),
            pltpu.SemaphoreType.DMA((coils // group,)),
            pltpu.SemaphoreType.DMA((coils // group,)),
            pltpu.SemaphoreType.DMA((2,)),
            pltpu.SemaphoreType.DMA((2,)),
        ],
        compiler_params=pltpu.CompilerParams(collective_id=0, has_side_effects=True),
        name="normal_operator",
    )(image, sensitivity, kernel, *consts)


def solution(mesh):
    return jax.shard_map(
        functools.partial(local, mesh.shape["slab"]),
        mesh=mesh,
        in_specs=(
            P(None, "slab", "scan", None),
            P("scan", None, "slab", None, None),
            P(None, "slab", None),
        ),
        out_specs=P(None, "slab", "scan", None),
        check_vma=False,
    )
```

```python
import functools
import math

import jax
import jax.numpy as jnp
import ml_dtypes
import numpy as np
from jax import lax
from jax.experimental import pallas as pl
from jax.experimental.pallas import tpu as pltpu
from jax.sharding import PartitionSpec as P

MESH = pl.DeviceIdType.MESH
smooth_weight = 0.1
group = 2


def factor(count_out, count_in, length, sign):
    phases = np.outer(np.arange(count_out), np.arange(count_in)) % length
    angles = phases.astype(np.float32) * np.float32(2.0 * math.pi / length)
    scale = np.float32(1.0 / math.sqrt(length))
    return np.cos(angles) * scale, sign * np.sin(angles) * scale


def stacked(real, imaginary):
    rows = np.stack([np.stack([real, -imaginary], 1), np.stack([imaginary, real], 1)])
    return rows.astype(ml_dtypes.bfloat16)


def tables(nx, ny, nz, gx, gy, gz):
    fx, fy, fz = (stacked(*factor(g, n, g, -1.0)) for n, g in ((nx, gx), (ny, gy), (nz, gz)))
    hx, hy, hz = (stacked(*factor(n, g, g, 1.0)) for n, g in ((nx, gx), (ny, gy), (nz, gz)))
    return (
        fy.transpose(1, 0, 2, 3).reshape(2 * gy, 2 * ny),
        fx.transpose(0, 1, 3, 2).reshape(2 * gx, 2 * nx),
        fz.transpose(2, 3, 0, 1).reshape(2 * nz, 2 * gz),
        hz.transpose(2, 3, 0, 1).reshape(2 * gz, 2 * nz),
        hx.transpose(1, 0, 2, 3).reshape(2 * nx, 2 * gx),
        hy.transpose(0, 1, 3, 2).reshape(2 * ny, 2 * gy),
    )


def dot(a, b):
    return jnp.dot(a, b, preferred_element_type=jnp.float32)


def body(
    n,
    image_hbm,
    maps_hbm,
    kernel_hbm,
    *refs,
):
    table_hbm, refs = refs[:6], refs[6:]
    (out, image, maps, weight, *refs) = refs
    table, refs = refs[:6], refs[6:]
    (lines, spectra, backs, planes, face, halo, total, load_sem, out_sem, in_sem, back_out_sem, back_in_sem, face_sem, halo_sem) = refs
    coils, _, ny, nz = maps.shape
    per = lines.shape[2]
    me = lax.axis_index("slab")

    loads = [pltpu.make_async_copy(image_hbm.at[:, 0], image, load_sem.at[0])]
    loads.append(pltpu.make_async_copy(maps_hbm.at[:, :, 0], maps, load_sem.at[1]))
    for i in range(6):
        loads.append(pltpu.make_async_copy(table_hbm[i], table[i], load_sem.at[2 + i]))
    for i in range(per):
        loads.append(pltpu.make_async_copy(kernel_hbm.at[:, i], weight.at[i], load_sem.at[8 + i]))
    for load in loads:
        load.start()

    barrier = pltpu.get_barrier_semaphore()

    def greet(k, carry):
        pl.semaphore_signal(
            barrier, inc=1, device_id={"slab": lax.rem(me + k, n)}, device_id_type=MESH
        )
        return carry

    lax.fori_loop(1, n, greet, 0, unroll=4)

    for load in loads[:3]:
        load.wait()
    face[...] = image[...].astype(face.dtype)

    def spread(c, carry):
        real, imaginary = maps[c, 0].astype(jnp.float32), maps[c, 1].astype(jnp.float32)
        coil_real = real * image[0] - imaginary * image[1]
        coil_imaginary = real * image[1] + imaginary * image[0]
        coil = jnp.concatenate([coil_real, coil_imaginary]).astype(jnp.bfloat16)
        along = dot(table[0][...], coil).astype(jnp.bfloat16)
        lines.at[c].reshape(n * per * 2, nz)[...] = along
        spectra[c, :, me] = lines[c, me]
        return carry

    lax.fori_loop(0, coils, spread, 0)
    pl.semaphore_wait(barrier, n - 1)

    def send(g, d):
        pltpu.make_async_remote_copy(
            lines.at[pl.ds(g * group, group), d],
            spectra.at[pl.ds(g * group, group), :, me],
            out_sem.at[g],
            in_sem.at[g],
            device_id={"slab": d},
            device_id_type=MESH,
        ).start()

    def send_back(g, d):
        pltpu.make_async_remote_copy(
            backs.at[pl.ds(g * group, group), :, d],
            planes.at[pl.ds(g * group, group), me],
            back_out_sem.at[g],
            back_in_sem.at[g],
            device_id={"slab": d},
            device_id_type=MESH,
        ).start()

    def each(act, g):
        def step(k, carry):
            act(g, lax.rem(me + k, n))
            return carry

        lax.fori_loop(1, n, step, 0, unroll=4)

    def face_copy(side):
        return pltpu.make_async_remote_copy(
            face,
            halo.at[side],
            face_sem.at[side],
            halo_sem.at[side],
            device_id={"slab": lax.rem(me + (1 if side == 0 else n - 1), n)},
            device_id_type=MESH,
        )

    @pl.when(me < n - 1)
    def _():
        face_copy(0).start()

    @pl.when(me > 0)
    def _():
        face_copy(1).start()

    groups = coils // group

    def start(g, carry):
        each(send, g)
        return carry

    lax.fori_loop(0, groups, start, 0)
    for load in loads[3:]:
        load.wait()

    def middle(c, carry):
        for i in range(per):
            x = spectra.at[c, i].reshape(2 * n, nz)[...]
            along = dot(table[1][...], x).astype(jnp.bfloat16)
            half = along.shape[0] // 2
            rows = jnp.concatenate([along[:half], along[half:]], axis=1)
            spectrum = dot(rows, table[2][...])
            gz = spectrum.shape[1] // 2
            k = weight[i]
            filtered = jnp.concatenate(
                [spectrum[:, :gz] * k, spectrum[:, gz:] * k], axis=1
            ).astype(jnp.bfloat16)
            back = dot(filtered, table[3][...]).astype(jnp.bfloat16)
            columns = jnp.concatenate([back[:, :nz], back[:, nz:]], axis=0)
            first = dot(table[4][...], columns).astype(jnp.bfloat16)
            backs.at[c, i].reshape(2 * n, nz)[...] = first
        planes[c, me] = backs[c, :, me]
        return carry

    def turn(g, carry):
        arrived = spectra.at[pl.ds(g * group, group), :, pl.ds(0, n - 1)]
        pltpu.make_async_copy(arrived, arrived, in_sem.at[g]).wait()
        lax.fori_loop(g * group, (g + 1) * group, middle, 0)
        each(send_back, g)
        return carry

    lax.fori_loop(0, groups, turn, 0)

    @pl.when(me > 0)
    def _():
        face_copy(0).wait_recv()

    @pl.when(me == 0)
    def _():
        halo[0] = jnp.zeros_like(halo[0])

    @pl.when(me < n - 1)
    def _():
        face_copy(1).wait_recv()

    @pl.when(me == n - 1)
    def _():
        halo[1] = jnp.zeros_like(halo[1])

    for p in range(2):
        plane = image[p]
        beside = halo[0, p].astype(jnp.float32) + halo[1, p].astype(jnp.float32)
        row, column = jnp.zeros((1, nz), jnp.float32), jnp.zeros((ny, 1), jnp.float32)
        beside += jnp.concatenate([plane[1:], row], axis=0) + jnp.concatenate([row, plane[:-1]], axis=0)
        beside += jnp.concatenate([plane[:, 1:], column], axis=1) + jnp.concatenate([column, plane[:, :-1]], axis=1)
        total[p] = smooth_weight * (6.0 * plane - beside)

    def finish(c, carry):
        coil = dot(table[5][...], planes.at[c].reshape(n * per * 2, nz)[...])
        coil_real, coil_imaginary = coil[:ny], coil[ny:]
        real, imaginary = maps[c, 0].astype(jnp.float32), maps[c, 1].astype(jnp.float32)
        total[0] += real * coil_real + imaginary * coil_imaginary
        total[1] += real * coil_imaginary - imaginary * coil_real
        return carry

    def gather(g, carry):
        arrived = planes.at[pl.ds(g * group, group), pl.ds(0, n - 1)]
        pltpu.make_async_copy(arrived, arrived, back_in_sem.at[g]).wait()
        return lax.fori_loop(g * group, (g + 1) * group, finish, carry)

    lax.fori_loop(0, groups, gather, 0)
    out[:, 0] = total[...]

    def drain(g, carry):
        left = lines.at[pl.ds(g * group, group), pl.ds(0, n - 1)]
        pltpu.make_async_copy(left, left, out_sem.at[g]).wait()
        pltpu.make_async_copy(left, left, back_out_sem.at[g]).wait()
        return carry

    lax.fori_loop(0, groups, drain, 0)

    @pl.when(me < n - 1)
    def _():
        face_copy(0).wait_send()

    @pl.when(me > 0)
    def _():
        face_copy(1).wait_send()


def local(n, image, sensitivity, kernel):
    coils, _, _, ny, nz = sensitivity.shape
    gx, per, gz = kernel.shape
    nx, gy = n, n * per
    consts = [jnp.asarray(t) for t in tables(nx, ny, nz, gx, gy, gz)]
    whole = pl.BlockSpec(memory_space=pl.ANY)
    half = jnp.bfloat16
    return pl.pallas_call(
        functools.partial(body, n),
        out_shape=jax.ShapeDtypeStruct(image.shape, image.dtype),
        in_specs=[whole] * 9,
        out_specs=pl.BlockSpec(memory_space=pltpu.VMEM),
        scratch_shapes=[
            pltpu.VMEM((2, ny, nz), jnp.float32),
            pltpu.VMEM((coils, 2, ny, nz), half),
            pltpu.VMEM((per, gx, gz), jnp.float32),
            *[pltpu.VMEM(t.shape, half) for t in consts],
            pltpu.VMEM((coils, n, per, 2, nz), half),
            pltpu.VMEM((coils, per, n, 2, nz), half),
            pltpu.VMEM((coils, per, n, 2, nz), half),
            pltpu.VMEM((coils, n, per, 2, nz), half),
            pltpu.VMEM((2, ny, nz), half),
            pltpu.VMEM((2, 2, ny, nz), half),
            pltpu.VMEM((2, ny, nz), jnp.float32),
            pltpu.SemaphoreType.DMA((8 + per,)),
            pltpu.SemaphoreType.DMA((coils // group,)),
            pltpu.SemaphoreType.DMA((coils // group,)),
            pltpu.SemaphoreType.DMA((coils // group,)),
            pltpu.SemaphoreType.DMA((coils // group,)),
            pltpu.SemaphoreType.DMA((2,)),
            pltpu.SemaphoreType.DMA((2,)),
        ],
        compiler_params=pltpu.CompilerParams(collective_id=0, has_side_effects=True),
        name="normal_operator",
    )(image, sensitivity, kernel, *consts)


def solution(mesh):
    return jax.shard_map(
        functools.partial(local, mesh.shape["slab"]),
        mesh=mesh,
        in_specs=(
            P(None, "slab", "scan", None),
            P("scan", None, "slab", None, None),
            P(None, "slab", None),
        ),
        out_specs=P(None, "slab", "scan", None),
        check_vma=False,
    )
```
